32 devices in a mesh: sfc: 8 (over z, x), grp: 4 (over y, core).
Axes of the slice: x: 2, y: 2, z: 4, core: 2. Of those that a mesh axis runs over, the one named last changes fastest.
Arguments:
- source: float32 [32, 16, 1024], P('sfc', None, 'grp'), may hold values from -8 to 8
- layer_counts: int32 [8], P('sfc'), may hold values from 1 to 4, 21 in all
Outputs:
- solution: float32 [32, 16, 1024], P('sfc', None, 'grp')
- residual: float32 [32, 16, 1024], P('sfc', None, 'grp')
- direction: float32 [32, 16, 1024], P('sfc', None, 'grp')
The draws below stay inside these ranges and needn't reach their ends.
Inputs may be any that keep to these rules, and one draw needn't show every extreme that they name: `layer_counts`: each entry counts the live leading slots of that index of sfc; they sum to 21, and at least one entry equals 4.
All inputs are finite; a program needn't handle non-finite values. No bound on the sum of `layer_counts` on one device may be relied on, other than what follows from the above.
Results may differ from the reference program's by a relative error of at most 0.00011.
Values sent between devices are 32-bit elements; how exact they have to be, the bound alone decides.
A program may use at most 64 MiB of HBM per device.

```python
import math
import jax
import jax.numpy as jnp
import numpy as np

E = 16
H = 8
BCAP = 4
PRE_SWEEPS = 2
POST_SWEEPS = 2
COARSE_SWEEPS = 4
SLOTS = 32
LIVE = 21
N_SFC = 8
N_GRP = 4


def draw_source(key, part):
    shape = (BCAP * N_SFC, E, N_GRP * E * E)
    slot = jnp.arange(BCAP * N_SFC, dtype=jnp.float32)
    device = jnp.floor(slot / BCAP)
    rise = (1.0 + 2.0 * device / max(N_SFC - 1, 1))[:, None, None]
    values = jax.random.normal(key, shape, jnp.float32) * rise
    return jnp.clip(values, -8.0, 8.0)


def profile(amount, total, reach, lean):
    portions = [(1 << 20) // math.isqrt(grade ** lean) + 1 for grade in range(2, amount + 1)]
    rest, given = total - reach - (amount - 1), [1] * (amount - 1)
    while rest > 0:
        free = [i for i in range(amount - 1) if given[i] < reach]
        whole, remaining = sum([portions[i] for i in free]), rest
        for i in free:
            extra = min(reach - given[i], max(1, remaining * portions[i] // whole), rest)
            given[i] = given[i] + extra
            rest = rest - extra
    return np.array([reach] + given)


def uneven_parts(own_key, amount, total, reach, slope):
    if amount == 2:
        one = jax.random.randint(own_key, (), max(1, total - reach), min(reach, total - 1) + 1)
        return jnp.stack([one, total - one])
    tallies = jnp.asarray(profile(amount, total, reach, slope), jnp.int32)
    twos = (amount - 1) // 2
    giver, sink = tallies[1:1 + 2 * twos:2], tallies[2:2 + 2 * twos:2]
    slack = jnp.minimum(giver - 1, reach - sink)
    shifted = jax.random.randint(jax.random.fold_in(own_key, 1), (twos,), 0, 1 << 20) % (slack + 1)
    tallies = tallies.at[1:1 + 2 * twos:2].set(giver - shifted).at[2:2 + 2 * twos:2].set(sink + shifted)
    return tallies[jax.random.permutation(jax.random.fold_in(own_key, 2), amount)]


def setup_inputs(seed: int = 0) -> dict:
    keys = jax.random.split(jax.random.key(seed), 3)
    return {
        "source": draw_source(jax.random.fold_in(keys[2], 71), 0),
        "layer_counts": uneven_parts(keys[1], N_SFC, LIVE, BCAP, 2).astype(jnp.int32),
    }


OMEGA = 2.0 / 3.0


def laplace(field, counts, edge):
    n_dev, planes, width = field.shape
    zero_plane = jnp.zeros((1, 1, width), jnp.float32)
    last_index = (counts * edge - 1).astype(jnp.int32)
    last = jnp.take_along_axis(field, last_index[:, None, None], axis=1)
    first = field[:, :1]
    prev_last = jnp.concatenate([zero_plane, last[:-1]], axis=0)
    next_first = jnp.concatenate([first[1:], zero_plane], axis=0)
    below = jnp.concatenate([prev_last, field[:, :-1]], axis=1)
    above = jnp.concatenate([field[:, 1:], jnp.zeros((n_dev, 1, width), jnp.float32)], axis=1)
    plane = jnp.arange(planes, dtype=jnp.int32)
    at_last = (plane[None, :] == last_index[:, None])[:, :, None]
    above = above + jnp.where(at_last, next_first, 0.0)
    pad_rows = jnp.zeros((n_dev, planes, edge), jnp.float32)
    north = jnp.concatenate([field[:, :, edge:], pad_rows], axis=2)
    south = jnp.concatenate([pad_rows, field[:, :, :-edge]], axis=2)
    column = (jnp.arange(width, dtype=jnp.int32) % edge)[None, None, :]
    pad_col = jnp.zeros((n_dev, planes, 1), jnp.float32)
    up_z = jnp.where(column != edge - 1, jnp.concatenate([field[:, :, 1:], pad_col], axis=2), 0.0)
    down_z = jnp.where(column != 0, jnp.concatenate([pad_col, field[:, :, :-1]], axis=2), 0.0)
    total = 6.0 * field - below - above - north - south - up_z - down_z
    live = (plane[None, :] < (counts * edge)[:, None])[:, :, None]
    return jnp.where(live, total, 0.0)


def restrict(field):
    n_dev, planes, width = field.shape
    across = width // (E * E) * E
    blocks = field.reshape(n_dev, planes // 2, 2, across // 2, 2, H, 2)
    return 0.125 * jnp.sum(blocks, axis=(2, 4, 6)).reshape(n_dev, planes // 2, (across // 2) * H)


def prolong(coarse):
    n_dev, planes, width = coarse.shape
    across = width // H
    blocks = coarse.reshape(n_dev, planes, 1, across, 1, H, 1)
    blocks = jnp.broadcast_to(blocks, (n_dev, planes, 2, across, 2, H, 2))
    return blocks.reshape(n_dev, planes * 2, across * 2 * H * 2)


def vcycle(rhs, counts):
    step = OMEGA / 6.0
    smooth = step * rhs
    for sweep in range(PRE_SWEEPS - 1):
        smooth = smooth + step * (rhs - laplace(smooth, counts, E))
    defect = rhs - laplace(smooth, counts, E)
    coarse_rhs = restrict(defect)
    coarse_step = OMEGA / 1.5
    correction = coarse_step * coarse_rhs
    for sweep in range(COARSE_SWEEPS - 1):
        correction = correction + coarse_step * (coarse_rhs - 0.25 * laplace(correction, counts, H))
    smooth = smooth + prolong(correction)
    for sweep in range(POST_SWEEPS):
        smooth = smooth + step * (rhs - laplace(smooth, counts, E))
    return smooth


def reference(source, layer_counts):
    width = source.shape[2]
    field = source.reshape(N_SFC, BCAP * E, width)
    plane = jnp.arange(BCAP * E, dtype=jnp.int32)
    live = (plane[None, :] < (layer_counts * E)[:, None])[:, :, None]
    first_rhs = jnp.where(live, field, 0.0)
    first_z = vcycle(first_rhs, layer_counts)
    image = laplace(first_z, layer_counts, E)
    rz_value = jnp.sum(first_rhs * first_z)
    curv = jnp.sum(first_z * image)
    alpha = rz_value / curv
    solution = alpha * first_z
    residual = first_rhs - alpha * image
    next_z = vcycle(residual, layer_counts)
    cross = jnp.sum(next_z * image)
    direction = next_z - (cross / curv) * first_z
    shape = (SLOTS, E, width)
    return solution.reshape(shape), residual.reshape(shape), direction.reshape(shape)
```

```python
import functools

import jax
import jax.numpy as jnp
from jax import lax
from jax.experimental import pallas as pl
from jax.experimental.pallas import tpu as pltpu
from jax.sharding import PartitionSpec as P

MESH = pl.DeviceIdType.MESH
OMEGA = 2.0 / 3.0
LANES = 128
SUBS = 8
COARSE_SWEEPS = 4
POST_SWEEPS = 2
WAYS = ((0, 1), (0, -1), (1, 0), (1, 1), (1, -1), (-1, 0), (-1, 1), (-1, -1))


def kernel(
    dims, count_ref, source_ref, solution_ref, residual_ref, direction_ref,
    rhs, smooth, other, coarse, ea, eb, mask, image_ref, first_ref, last,
    side, below, above, part, total, red_grp, red_sfc,
    send_sem, recv_sem, grp_send, grp_recv, sfc_send, sfc_recv,
):
    slots, edge, tiles, n_sfc, n_grp = dims
    planes = slots * edge
    sfc = lax.axis_index("sfc")
    grp = lax.axis_index("grp")
    count = count_ref[0]
    step = OMEGA / 6.0
    cstep = OMEGA / 1.5
    middle = (SUBS - tiles) // 2

    def there(ds, dg):
        flag = None
        if ds:
            flag = sfc < n_sfc - 1 if ds > 0 else sfc > 0
        if dg:
            extra = grp < n_grp - 1 if dg > 0 else grp > 0
            flag = extra if flag is None else jnp.logical_and(flag, extra)
        return flag

    barrier = pltpu.get_barrier_semaphore()

    def greet(i, axis, size, me):
        pl.semaphore_signal(
            barrier, inc=1, device_id={axis: lax.rem(me + i, size)}, device_id_type=MESH
        )

    for i in range(1, n_grp):
        greet(i, "grp", n_grp, grp)

    def greet_sfc(i, carry):
        greet(i, "sfc", n_sfc, sfc)
        return carry

    lax.fori_loop(1, n_sfc, greet_sfc, 0)
    for ds, dg in WAYS:
        if ds and dg:
            @pl.when(there(ds, dg))
            def _():
                pl.semaphore_signal(
                    barrier, inc=1, device_id={"sfc": sfc + ds, "grp": grp + dg},
                    device_id_type=MESH,
                )

    def one(flag):
        return jnp.where(flag, 1, 0)

    diagonals = (one(sfc > 0) + one(sfc < n_sfc - 1)) * (one(grp > 0) + one(grp < n_grp - 1))

    lane = lax.broadcasted_iota(jnp.int32, (1, SUBS, LANES), 2)
    sub = lax.broadcasted_iota(jnp.int32, (1, SUBS, LANES), 1)
    z = lane % edge

    def has(flag_int):
        return flag_int > 0

    has_below = one(sfc > 0)
    has_above = one(sfc < n_sfc - 1)
    has_left = one(grp > 0)
    has_right = one(grp < n_grp - 1)
    owned = jnp.logical_and(sub >= middle, sub < middle + tiles)
    lefts = jnp.logical_and(sub >= middle - tiles, sub < middle)
    rights = jnp.logical_and(sub >= middle + tiles, sub < middle + 2 * tiles)
    rows_ok = (
        jnp.where(owned, 1, 0) + jnp.where(lefts, 1, 0) * has_left
        + jnp.where(rights, 1, 0) * has_right
    )
    for s in range(slots + 2):
        if s == 0:
            ok = has_below
        else:
            ok = one(count >= s) + one(count == s - 1) * has_above
        mask[pl.ds(SUBS * s, SUBS), :] = (rows_ok * ok).astype(jnp.float32)[0]

    def zero_rhs(i, carry):
        rhs[pl.ds(i * SUBS, SUBS), :] = jnp.zeros((SUBS, LANES), jnp.float32)
        return carry

    lax.fori_loop(0, planes + 2 * edge + 2, zero_rhs, 0)

    def fill_last(src):
        value = src[pl.ds(0, edge), :]
        for s in range(1, slots):
            value = jnp.where(count > s, src[pl.ds(s * edge, edge), :], value)
        last[...] = value

    def copies(e, i, ds, dg, src):
        gpos = 1 - dg
        if ds == 0:
            source, target = src, side.at[e, gpos // 2]
        elif ds > 0:
            source, target = last.at[e], below.at[e, gpos]
        else:
            source, target = src.at[pl.ds(0, edge)], above.at[e, gpos]
        return pltpu.make_async_remote_copy(
            src_ref=source, dst_ref=target, send_sem=send_sem.at[e, i],
            recv_sem=recv_sem.at[e, i], device_id={"sfc": sfc + ds, "grp": grp + dg},
            device_id_type=MESH,
        )

    def start(e, src):
        for i, (ds, dg) in enumerate(WAYS):
            @pl.when(there(ds, dg))
            def _(i=i, ds=ds, dg=dg):
                copies(e, i, ds, dg, src).start()

    def receive(e, src):
        for i, (ds, dg) in enumerate(WAYS):
            @pl.when(there(-ds, -dg))
            def _(i=i, ds=ds, dg=dg):
                copies(e, i, ds, dg, src).wait_recv()

    def sent(e, src):
        for i, (ds, dg) in enumerate(WAYS):
            @pl.when(there(ds, dg))
            def _(i=i, ds=ds, dg=dg):
                copies(e, i, ds, dg, src).wait_send()

    def pick_last(e, src):
        value = src[pl.ds(0, edge), :]
        for s in range(1, slots):
            value = jnp.where(count > s, src[pl.ds(s * edge, edge), :], value)
        last[e] = value

    def unpack(e, src):
        sides = ((0, has_left), (1, 1), (2, has_right))
        for g, present in sides:
            for s in range(slots + 2):
                for h in range(edge // SUBS):
                    for t in range(tiles):
                        cols = pl.ds(t * LANES, LANES)
                        rows = pl.ds(h * SUBS, SUBS)

                        def centre(slot):
                            at = pl.ds(slot * edge + h * SUBS, SUBS)
                            return src[at, cols] if g == 1 else side[e, g // 2, at, cols]

                        if s == 0:
                            value = jnp.where(has(has_below * present), below[e, g, rows, cols], 0.0)
                        else:
                            up = one(count == s - 1) * has_above * present
                            value = jnp.zeros((SUBS, LANES), jnp.float32)
                            if s >= 2:
                                value = jnp.where(has(up), above[e, g, rows, cols], value)
                            if s <= slots:
                                value = jnp.where(has(one(count >= s) * present), centre(s - 1), value)
                        plane = 1 + s * edge + h * SUBS
                        at_sub = middle + (g - 1) * tiles + t
                        rhs[pl.ds(plane * SUBS + at_sub, SUBS, stride=SUBS), :] = value

    def roll(v, amount, axis):
        return pltpu.roll(v, amount % v.shape[axis], axis)

    def inplane(v, dz, dy):
        up_z = jnp.where(z < edge - dz, roll(v, -dz, 2), 0.0)
        down_z = jnp.where(z >= dz, roll(v, dz, 2), 0.0)
        ru = roll(v, -dy, 2)
        up_y = jnp.where(lane < LANES - dy, ru, roll(ru, -1, 1))
        rd = roll(v, dy, 2)
        down_y = jnp.where(lane >= dy, rd, roll(rd, 1, 1))
        return (up_z + down_z) + (up_y + down_y)

    def load(ref, p, n):
        return ref[pl.ds((p + 1) * SUBS, n * SUBS), :].reshape(n, SUBS, LANES)

    def store(ref, p, value):
        n = value.shape[0]
        ref[pl.ds((p + 1) * SUBS, n * SUBS), :] = value.reshape(n * SUBS, LANES)

    def lap(ref, p, n, dz=1, dy=edge):
        wide = load(ref, p - 1, n + 2)
        v = wide[1:-1]
        return v, 6.0 * v - (wide[:-2] + wide[2:]) - inplane(v, dz, dy)

    def slot_mask(s):
        return mask[pl.ds(SUBS * s, SUBS), :][None]

    chunk = SUBS
    per_slot = edge // chunk
    chunks = (slots + 2) * per_slot

    def vcycle(result):
        for c in range(chunks):
            r, applied = lap(rhs, c * chunk, chunk)
            store(smooth, c * chunk, slot_mask(c // per_slot) * (2.0 * step * r - step * step * applied))
        for c in range(chunks):
            v, applied = lap(smooth, c * chunk, chunk)
            q = load(rhs, c * chunk, chunk) - applied
            q = q.reshape(chunk // 2, 2, SUBS, LANES)
            q = q[:, 0] + q[:, 1]
            q = q + jnp.where(lane % 2 == 0, roll(q, -1, 2), roll(q, 1, 2))
            q = q + jnp.where(lane // edge % 2 == 0, roll(q, -edge, 2), roll(q, edge, 2))
            store(coarse, c * chunk // 2, slot_mask(c // per_slot) * (0.125 * q))
        half = edge // 2
        for s in range(slots + 2):
            v, applied = lap(coarse, s * half, half, 2, 2 * edge)
            store(ea, s * half, slot_mask(s) * (2.0 * cstep * v - 0.25 * cstep * cstep * applied))
        now, then = ea, eb
        for sweep in range(COARSE_SWEEPS - 2):
            for s in range(slots + 2):
                v, applied = lap(now, s * half, half, 2, 2 * edge)
                c = load(coarse, s * half, half)
                value = slot_mask(s) * (v + cstep * (c - 0.25 * applied))
                store(then, s * half, value)
            now, then = then, now
        for c in range(1, chunks - 1):
            e = load(now, c * chunk // 2, chunk // 2)[:, None]
            e = jnp.broadcast_to(e, (chunk // 2, 2, SUBS, LANES)).reshape(chunk, SUBS, LANES)
            store(smooth, c * chunk, load(smooth, c * chunk, chunk) + e)
        now, then = smooth, other
        for sweep in range(POST_SWEEPS):
            for c in range(1, chunks - 1):
                v, applied = lap(now, c * chunk, chunk)
                r = load(rhs, c * chunk, chunk)
                store(then, c * chunk, slot_mask(c // per_slot) * (v + step * (r - applied)))
            now, then = then, now
        return now

    def natural(ref, s, h, t):
        plane = 1 + (s + 1) * edge + h * SUBS
        return ref[pl.ds(plane * SUBS + middle + t, SUBS, stride=SUBS), :]

    def owned_tiles():
        for s in range(slots):
            for h in range(edge // SUBS):
                for t in range(tiles):
                    yield s, h, t, pl.ds(s * edge + h * SUBS, SUBS), pl.ds(t * LANES, LANES)

    pick_last(0, source_ref)
    pl.semaphore_wait(barrier, n_grp - 1 + n_sfc - 1 + diagonals)
    start(0, source_ref)
    receive(0, source_ref)
    unpack(0, source_ref)
    z0 = vcycle(None)
    for c in range(per_slot, chunks - per_slot):
        _, applied = lap(z0, c * chunk, chunk)
        store(other, c * chunk, applied)
    acc_rz = jnp.zeros((SUBS, LANES), jnp.float32)
    acc_curv = jnp.zeros((SUBS, LANES), jnp.float32)
    for s, h, t, rows, cols in owned_tiles():
        value = natural(z0, s, h, t)
        image = natural(other, s, h, t)
        source = source_ref[rows, cols]
        if s:
            value = jnp.where(count > s, value, 0.0)
            image = jnp.where(count > s, image, 0.0)
            source = jnp.where(count > s, source, 0.0)
        first_ref[rows, cols] = value
        image_ref[rows, cols] = image
        acc_rz = acc_rz + source * value
        acc_curv = acc_curv + value * image
    pick_last(1, image_ref)
    start(1, image_ref)
    receive(1, image_ref)
    unpack(1, image_ref)
    w = vcycle(None)
    acc_s = jnp.zeros((SUBS, LANES), jnp.float32)
    for s, h, t, rows, cols in owned_tiles():
        value = natural(w, s, h, t)
        if s:
            value = jnp.where(count > s, value, 0.0)
        direction_ref[rows, cols] = value
        acc_s = acc_s + value * image_ref[rows, cols]

    sums = [jnp.sum(a, axis=0, keepdims=True) for a in (acc_rz, acc_curv, acc_s)]
    sums = sums + [jnp.zeros((SUBS - 3, LANES), jnp.float32)]
    part[...] = jnp.concatenate(sums, axis=0)

    def reduce(src, dst, axis, size, me, send, recv):
        def copy(slot, target):
            return pltpu.make_async_remote_copy(
                src_ref=src, dst_ref=dst.at[slot], send_sem=send.at[target],
                recv_sem=recv.at[slot], device_id={axis: target}, device_id_type=MESH,
            )

        def go(i, carry):
            copy(me, lax.rem(me + i, size)).start()
            return carry

        lax.fori_loop(1, size, go, 0)
        dst[me] = src[...]

        def got(i, carry):
            j = lax.rem(me + i, size)
            copy(j, j).wait_recv()
            return carry

        lax.fori_loop(1, size, got, 0)

        def add(i, acc):
            return acc + dst[i]

        return lax.fori_loop(0, size, add, jnp.zeros((SUBS, LANES), jnp.float32))

    def done(src, dst, axis, size, me, send, recv):
        def out(i, carry):
            j = lax.rem(me + i, size)
            pltpu.make_async_remote_copy(
                src_ref=src, dst_ref=dst.at[me], send_sem=send.at[j],
                recv_sem=recv.at[me], device_id={axis: j}, device_id_type=MESH,
            ).wait_send()
            return carry

        lax.fori_loop(1, size, out, 0)

    by_grp = (part, red_grp, "grp", n_grp, grp, grp_send, grp_recv)
    by_sfc = (total, red_sfc, "sfc", n_sfc, sfc, sfc_send, sfc_recv)
    total[...] = reduce(*by_grp)
    grand = jnp.sum(reduce(*by_sfc), axis=1, keepdims=True)
    rz, curv, cross = grand[0:1], grand[1:2], grand[2:3]
    alpha = rz / curv
    ratio = cross / curv
    for s, h, t, rows, cols in owned_tiles():
        source = source_ref[rows, cols]
        if s:
            source = jnp.where(count > s, source, 0.0)
        first = first_ref[rows, cols]
        solution_ref[rows, cols] = alpha * first
        residual_ref[rows, cols] = source - alpha * image_ref[rows, cols]
        direction_ref[rows, cols] = alpha * (ratio * first - direction_ref[rows, cols])
    sent(0, source_ref)
    sent(1, image_ref)
    done(*by_grp)
    done(*by_sfc)


def shards(n_sfc, n_grp, source, layer_counts):
    slots, edge, width = source.shape
    planes, tiles = slots * edge, width // LANES
    padded = (planes + 2 * edge + 2) * SUBS
    half_padded = ((slots + 2) * edge // 2 + 2) * SUBS
    f32 = jnp.float32
    vmem = pltpu.VMEM
    dma = pltpu.SemaphoreType.DMA
    out = jax.ShapeDtypeStruct((planes, width), f32)
    outs = pl.pallas_call(
        functools.partial(kernel, (slots, edge, tiles, n_sfc, n_grp)),
        out_shape=(out, out, out),
        in_specs=[
            pl.BlockSpec(memory_space=pltpu.SMEM),
            pl.BlockSpec(memory_space=pltpu.VMEM),
        ],
        out_specs=[pl.BlockSpec(memory_space=pltpu.VMEM)] * 3,
        scratch_shapes=[
            vmem((padded, LANES), f32),
            vmem((padded, LANES), f32),
            vmem((padded, LANES), f32),
            vmem((half_padded, LANES), f32),
            vmem((half_padded, LANES), f32),
            vmem((half_padded, LANES), f32),
            vmem(((slots + 2) * SUBS, LANES), f32),
            vmem((planes, width), f32),
            vmem((planes, width), f32),
            vmem((2, edge, width), f32),
            vmem((2, 2, planes, width), f32),
            vmem((2, 3, edge, width), f32),
            vmem((2, 3, edge, width), f32),
            vmem((SUBS, LANES), f32),
            vmem((SUBS, LANES), f32),
            vmem((n_grp, SUBS, LANES), f32),
            vmem((n_sfc, SUBS, LANES), f32),
            dma((2, len(WAYS))),
            dma((2, len(WAYS))),
            dma((n_grp,)),
            dma((n_grp,)),
            dma((n_sfc,)),
            dma((n_sfc,)),
        ],
        compiler_params=pltpu.CompilerParams(collective_id=0, has_side_effects=True),
        name="pcg",
    )(layer_counts, source.reshape(planes, width))
    return tuple(o.reshape(source.shape) for o in outs)


def solution(mesh):
    n_sfc, n_grp = mesh.shape["sfc"], mesh.shape["grp"]
    return jax.shard_map(
        functools.partial(shards, n_sfc, n_grp),
        mesh=mesh,
        in_specs=(P("sfc", None, "grp"), P("sfc")),
        out_specs=(P("sfc", None, "grp"), P("sfc", None, "grp"), P("sfc", None, "grp")),
        check_vma=False,
    )
```

```python
import functools

import jax
import jax.numpy as jnp
from jax import lax
from jax.experimental import pallas as pl
from jax.experimental.pallas import tpu as pltpu
from jax.sharding import PartitionSpec as P

MESH = pl.DeviceIdType.MESH
OMEGA = 2.0 / 3.0
LANES = 128
SUBS = 8
COARSE_SWEEPS = 4
POST_SWEEPS = 2
WAYS = ((0, 1), (0, -1), (1, 0), (1, 1), (1, -1), (-1, 0), (-1, 1), (-1, -1))


def kernel(
    dims, count_hbm, source_hbm, first_ref, image_ref, w_ref, source_out, scale_ref,
    source_ref, image_buf, counts, rhs, smooth, other, coarse, ea, eb, mask, own, last,
    side, below, above, part, red, local_sem,
    send_sem, recv_sem, red_send, red_recv,
):
    slots, edge, tiles, n_sfc, n_grp = dims
    planes = slots * edge
    sfc = lax.axis_index("sfc")
    grp = lax.axis_index("grp")
    me = sfc * n_grp + grp
    everyone = n_sfc * n_grp
    step = OMEGA / 6.0
    cstep = OMEGA / 1.5
    middle = (SUBS - tiles) // 2

    def there(ds, dg):
        flag = None
        if ds:
            flag = sfc < n_sfc - 1 if ds > 0 else sfc > 0
        if dg:
            extra = grp < n_grp - 1 if dg > 0 else grp > 0
            flag = extra if flag is None else jnp.logical_and(flag, extra)
        return flag

    barrier = pltpu.get_barrier_semaphore()

    def place(i):
        peer = lax.rem(me + i, everyone)
        return peer, {"sfc": peer // n_grp, "grp": lax.rem(peer, n_grp)}

    def greet(i, carry):
        pl.semaphore_signal(barrier, inc=1, device_id=place(i)[1], device_id_type=MESH)
        return carry

    count_copy = pltpu.make_async_copy(count_hbm, counts, local_sem.at[0])
    source_copy = pltpu.make_async_copy(source_hbm, source_ref, local_sem.at[1])
    count_copy.start()
    source_copy.start()
    lax.fori_loop(1, everyone, greet, 0)

    def one(flag):
        return jnp.where(flag, 1, 0)

    lane = lax.broadcasted_iota(jnp.int32, (1, SUBS, LANES), 2)
    sub = lax.broadcasted_iota(jnp.int32, (1, SUBS, LANES), 1)
    z = lane % edge

    def has(flag_int):
        return flag_int > 0

    has_below = one(sfc > 0)
    has_above = one(sfc < n_sfc - 1)
    has_left = one(grp > 0)
    has_right = one(grp < n_grp - 1)
    owned = jnp.logical_and(sub >= middle, sub < middle + tiles)
    lefts = jnp.logical_and(sub >= middle - tiles, sub < middle)
    rights = jnp.logical_and(sub >= middle + tiles, sub < middle + 2 * tiles)
    rows_ok = (
        jnp.where(owned, 1, 0) + jnp.where(lefts, 1, 0) * has_left
        + jnp.where(rights, 1, 0) * has_right
    )
    def zero_rhs(i, carry):
        rhs[pl.ds(i * SUBS, SUBS), :] = jnp.zeros((SUBS, LANES), jnp.float32)
        return carry

    lax.fori_loop(0, planes + 2 * edge + 2, zero_rhs, 0)

    count_copy.wait()
    count = counts[0]
    for s in range(slots + 2):
        if s == 0:
            ok = has_below
        else:
            ok = one(count >= s) + one(count == s - 1) * has_above
        mask[pl.ds(SUBS * s, SUBS), :] = (rows_ok * ok).astype(jnp.float32)[0]

    for s in range(slots):
        mine = jnp.where(owned, 1, 0) * one(count > s)
        own[pl.ds(SUBS * s, SUBS), :] = mine.astype(jnp.float32)[0]

    def copies(e, i, ds, dg, src):
        gpos = 1 - dg
        if ds == 0:
            source, target = src, side.at[e, gpos // 2]
        elif ds > 0:
            source, target = last.at[e], below.at[e, gpos]
        else:
            source, target = src.at[pl.ds(0, edge)], above.at[e, gpos]
        return pltpu.make_async_remote_copy(
            src_ref=source, dst_ref=target, send_sem=send_sem.at[e, i],
            recv_sem=recv_sem.at[e, i], device_id={"sfc": sfc + ds, "grp": grp + dg},
            device_id_type=MESH,
        )

    def start(e, src):
        for i, (ds, dg) in enumerate(WAYS):
            @pl.when(there(ds, dg))
            def _(i=i, ds=ds, dg=dg):
                copies(e, i, ds, dg, src).start()

    def receive(e, src):
        for i, (ds, dg) in enumerate(WAYS):
            @pl.when(there(-ds, -dg))
            def _(i=i, ds=ds, dg=dg):
                copies(e, i, ds, dg, src).wait_recv()

    def sent(e, src):
        for i, (ds, dg) in enumerate(WAYS):
            @pl.when(there(ds, dg))
            def _(i=i, ds=ds, dg=dg):
                copies(e, i, ds, dg, src).wait_send()

    def pick_last(e, src):
        value = src[pl.ds(0, edge), :]
        for s in range(1, slots):
            value = jnp.where(count > s, src[pl.ds(s * edge, edge), :], value)
        last[e] = value

    def unpack(e, src):
        sides = ((0, has_left), (1, 1), (2, has_right))
        for g, present in sides:
            for s in range(slots + 2):
                for h in range(edge // SUBS):
                    for t in range(tiles):
                        cols = pl.ds(t * LANES, LANES)
                        rows = pl.ds(h * SUBS, SUBS)

                        def centre(slot):
                            at = pl.ds(slot * edge + h * SUBS, SUBS)
                            return src[at, cols] if g == 1 else side[e, g // 2, at, cols]

                        if s == 0:
                            value = jnp.where(has(has_below * present), below[e, g, rows, cols], 0.0)
                        else:
                            up = one(count == s - 1) * has_above * present
                            value = jnp.zeros((SUBS, LANES), jnp.float32)
                            if s >= 2:
                                value = jnp.where(has(up), above[e, g, rows, cols], value)
                            if s <= slots:
                                value = jnp.where(has(one(count >= s) * present), centre(s - 1), value)
                        plane = 1 + s * edge + h * SUBS
                        at_sub = middle + (g - 1) * tiles + t
                        rhs[pl.ds(plane * SUBS + at_sub, SUBS, stride=SUBS), :] = value

    def roll(v, amount, axis):
        return pltpu.roll(v, amount % v.shape[axis], axis)

    def inplane(v, dz, dy):
        up_z = jnp.where(z < edge - dz, roll(v, -dz, 2), 0.0)
        down_z = jnp.where(z >= dz, roll(v, dz, 2), 0.0)
        ru = roll(v, -dy, 2)
        up_y = jnp.where(lane < LANES - dy, ru, roll(ru, -1, 1))
        rd = roll(v, dy, 2)
        down_y = jnp.where(lane >= dy, rd, roll(rd, 1, 1))
        return (up_z + down_z) + (up_y + down_y)

    def load(ref, p, n):
        return ref[pl.ds((p + 1) * SUBS, n * SUBS), :].reshape(n, SUBS, LANES)

    def store(ref, p, value):
        n = value.shape[0]
        ref[pl.ds((p + 1) * SUBS, n * SUBS), :] = value.reshape(n * SUBS, LANES)

    def lap(ref, p, n, dz=1, dy=edge):
        wide = load(ref, p - 1, n + 2)
        v = wide[1:-1]
        return v, 6.0 * v - (wide[:-2] + wide[2:]) - inplane(v, dz, dy)

    def slot_mask(s):
        return mask[pl.ds(SUBS * s, SUBS), :][None]

    chunk = SUBS
    per_slot = edge // chunk
    chunks = (slots + 2) * per_slot

    def vcycle(on_sum=None):
        acc = jnp.zeros((SUBS, LANES), jnp.float32)
        for c in range(chunks):
            r, applied = lap(rhs, c * chunk, chunk)
            store(smooth, c * chunk, slot_mask(c // per_slot) * (2.0 * step * r - step * step * applied))
        for c in range(chunks):
            v, applied = lap(smooth, c * chunk, chunk)
            r = load(rhs, c * chunk, chunk)
            q = r - applied
            s = c // per_slot - 1
            if on_sum is not None and 0 <= s < slots:
                acc = acc + own[pl.ds(SUBS * s, SUBS), :] * jnp.sum((r + q) * v, axis=0)
            q = q.reshape(chunk // 2, 2, SUBS, LANES)
            q = q[:, 0] + q[:, 1]
            q = q + jnp.where(lane % 2 == 0, roll(q, -1, 2), roll(q, 1, 2))
            q = q + jnp.where(lane // edge % 2 == 0, roll(q, -edge, 2), roll(q, edge, 2))
            store(coarse, c * chunk // 2, slot_mask(c // per_slot) * (0.125 * q))
        half = edge // 2
        for s in range(slots + 2):
            v, applied = lap(coarse, s * half, half, 2, 2 * edge)
            store(ea, s * half, slot_mask(s) * (2.0 * cstep * v - 0.25 * cstep * cstep * applied))
        now, then = ea, eb
        for sweep in range(COARSE_SWEEPS - 2):
            for s in range(slots + 2):
                v, applied = lap(now, s * half, half, 2, 2 * edge)
                c = load(coarse, s * half, half)
                value = slot_mask(s) * (v + cstep * (c - 0.25 * applied))
                store(then, s * half, value)
            now, then = then, now
        if on_sum is not None:
            for s in range(slots):
                ce = load(coarse, (s + 1) * half, half) * load(now, (s + 1) * half, half)
                acc = acc + own[pl.ds(SUBS * s, SUBS), :] * (2.0 * jnp.sum(ce, axis=0))
            on_sum(acc)
        for c in range(1, chunks - 1):
            e = load(now, c * chunk // 2, chunk // 2)[:, None]
            e = jnp.broadcast_to(e, (chunk // 2, 2, SUBS, LANES)).reshape(chunk, SUBS, LANES)
            store(smooth, c * chunk, load(smooth, c * chunk, chunk) + e)
        now, then = smooth, other
        for sweep in range(POST_SWEEPS):
            for c in range(1, chunks - 1):
                v, applied = lap(now, c * chunk, chunk)
                r = load(rhs, c * chunk, chunk)
                store(then, c * chunk, slot_mask(c // per_slot) * (v + step * (r - applied)))
            now, then = then, now
        return now

    def natural(ref, s, h, t):
        plane = 1 + (s + 1) * edge + h * SUBS
        return ref[pl.ds(plane * SUBS + middle + t, SUBS, stride=SUBS), :]

    def owned_tiles():
        for s in range(slots):
            for h in range(edge // SUBS):
                for t in range(tiles):
                    yield s, h, t, pl.ds(s * edge + h * SUBS, SUBS), pl.ds(t * LANES, LANES)

    source_copy.wait()
    pick_last(0, source_ref)
    pl.semaphore_wait(barrier, everyone - 1)
    start(0, source_ref)
    receive(0, source_ref)
    unpack(0, source_ref)
    z0 = vcycle()
    for c in range(per_slot, chunks - per_slot):
        _, applied = lap(z0, c * chunk, chunk)
        store(other, c * chunk, applied)
    acc_rz = jnp.zeros((SUBS, LANES), jnp.float32)
    acc_curv = jnp.zeros((SUBS, LANES), jnp.float32)
    for s, h, t, rows, cols in owned_tiles():
        value = natural(z0, s, h, t)
        image = natural(other, s, h, t)
        source = source_ref[rows, cols]
        if s:
            value = jnp.where(count > s, value, 0.0)
            image = jnp.where(count > s, image, 0.0)
            source = jnp.where(count > s, source, 0.0)
        first_ref[rows, cols] = value
        image_ref[rows, cols] = image
        image_buf[rows, cols] = image
        source_out[rows, cols] = source
        acc_rz = acc_rz + source * value
        acc_curv = acc_curv + value * image
    pick_last(1, image_buf)
    start(1, image_buf)
    row = lax.broadcasted_iota(jnp.int32, (1, LANES), 1)

    def whole(acc):
        return jnp.sum(jnp.sum(acc, axis=0, keepdims=True), axis=1, keepdims=True)

    rz, curv = whole(acc_rz), whole(acc_curv)
    known = jnp.where(row == 0, rz, jnp.where(row == 1, curv, 0.0))
    receive(1, image_buf)
    unpack(1, image_buf)

    def send(slot, peer, device):
        return pltpu.make_async_remote_copy(
            src_ref=part, dst_ref=red.at[slot], send_sem=red_send.at[peer],
            recv_sem=red_recv.at[slot], device_id=device, device_id_type=MESH,
        )

    def spread(acc):
        value = jnp.where(row == 2, whole(acc), known)
        part[...] = value
        red[me] = value

        def go(i, carry):
            peer, device = place(i)
            send(me, peer, device).start()
            return carry

        lax.fori_loop(1, everyone, go, 0)

    w = vcycle(spread)
    for s, h, t, rows, cols in owned_tiles():
        value = natural(w, s, h, t)
        if s:
            value = jnp.where(count > s, value, 0.0)
        w_ref[rows, cols] = value
    sent(0, source_ref)
    sent(1, image_buf)

    def got(i, carry):
        peer, device = place(i)
        send(peer, peer, device).wait_recv()
        return carry

    lax.fori_loop(1, everyone, got, 0)
    sums = jnp.sum(red[...], axis=0)

    def pick(i):
        return jnp.sum(jnp.where(row == i, sums, 0.0), axis=1, keepdims=True)

    alpha = pick(0) / pick(1)
    ratio = pick(2) / pick(1)
    scale_ref[...] = jnp.concatenate(
        [jnp.broadcast_to(alpha, (1, LANES)), jnp.broadcast_to(ratio, (1, LANES))], axis=0
    )

    def out(i, carry):
        peer, device = place(i)
        send(me, peer, device).wait_send()
        return carry

    lax.fori_loop(1, everyone, out, 0)


def combine(first, image, w, source, scale, solution_ref, residual_ref, direction_ref):
    alpha = scale[0:1, 0:1]
    ratio = scale[1:2, 0:1]
    solution_ref[...] = alpha * first[...]
    residual_ref[...] = source[...] - alpha * image[...]
    direction_ref[...] = alpha * (ratio * first[...] - w[...])


def shards(n_sfc, n_grp, source, layer_counts):
    slots, edge, width = source.shape
    planes, tiles = slots * edge, width // LANES
    padded = (planes + 2 * edge + 2) * SUBS
    half_padded = ((slots + 2) * edge // 2 + 2) * SUBS
    f32 = jnp.float32
    vmem = pltpu.VMEM
    dma = pltpu.SemaphoreType.DMA
    n = n_sfc * n_grp
    out = jax.ShapeDtypeStruct((planes, width), f32)
    parts = pl.pallas_call(
        functools.partial(kernel, (slots, edge, tiles, n_sfc, n_grp)),
        out_shape=(out, out, out, out, jax.ShapeDtypeStruct((2, LANES), f32)),
        in_specs=[pl.BlockSpec(memory_space=pl.ANY)] * 2,
        out_specs=[pl.BlockSpec(memory_space=pltpu.VMEM)] * 5,
        scratch_shapes=[
            vmem((planes, width), f32),
            vmem((planes, width), f32),
            pltpu.SMEM((1,), jnp.int32),
            vmem((padded, LANES), f32),
            vmem((padded, LANES), f32),
            vmem((padded, LANES), f32),
            vmem((half_padded, LANES), f32),
            vmem((half_padded, LANES), f32),
            vmem((half_padded, LANES), f32),
            vmem(((slots + 2) * SUBS, LANES), f32),
            vmem((slots * SUBS, LANES), f32),
            vmem((2, edge, width), f32),
            vmem((2, 2, planes, width), f32),
            vmem((2, 3, edge, width), f32),
            vmem((2, 3, edge, width), f32),
            vmem((1, LANES), f32),
            vmem((n, 1, LANES), f32),
            dma((2,)),
            dma((2, len(WAYS))),
            dma((2, len(WAYS))),
            dma((n,)),
            dma((n,)),
        ],
        compiler_params=pltpu.CompilerParams(
            collective_id=0, has_side_effects=True, vmem_limit_bytes=16 * 1024 * 1024
        ),
        name="pcg",
    )(layer_counts, source.reshape(planes, width))
    outs = pl.pallas_call(
        combine,
        out_shape=(out, out, out),
        in_specs=[pl.BlockSpec(memory_space=pltpu.VMEM)] * 5,
        out_specs=[pl.BlockSpec(memory_space=pltpu.VMEM)] * 3,
        compiler_params=pltpu.CompilerParams(vmem_limit_bytes=16 * 1024 * 1024),
        name="combine",
    )(*parts)
    return tuple(o.reshape(source.shape) for o in outs)


def solution(mesh):
    n_sfc, n_grp = mesh.shape["sfc"], mesh.shape["grp"]
    return jax.shard_map(
        functools.partial(shards, n_sfc, n_grp),
        mesh=mesh,
        in_specs=(P("sfc", None, "grp"), P("sfc")),
        out_specs=(P("sfc", None, "grp"), P("sfc", None, "grp"), P("sfc", None, "grp")),
        check_vma=False,
    )
```

```python
import functools

import jax
import jax.numpy as jnp
from jax import lax
from jax.experimental import pallas as pl
from jax.experimental.pallas import tpu as pltpu
from jax.sharding import PartitionSpec as P

MESH = pl.DeviceIdType.MESH
OMEGA = 2.0 / 3.0
LANES = 128
SUBS = 8
COARSE_SWEEPS = 4
POST_SWEEPS = 2
WAYS = ((0, 1), (0, -1), (1, 0), (1, 1), (1, -1), (-1, 0), (-1, 1), (-1, -1))


def kernel(
    dims, count_hbm, source_hbm, first_ref, image_ref, w_ref, source_out, scale_ref,
    source_ref, image_buf, counts, rhs, smooth, other, coarse, ea, eb, mask, own, packed,
    side, below, above, part, red, local_sem,
    send_sem, recv_sem, red_send, red_recv, hello,
):
    slots, edge, tiles, n_sfc, n_grp = dims
    planes = slots * edge
    sfc = lax.axis_index("sfc")
    grp = lax.axis_index("grp")
    me = sfc * n_grp + grp
    everyone = n_sfc * n_grp
    step = OMEGA / 6.0
    cstep = OMEGA / 1.5
    middle = (SUBS - tiles) // 2

    def there(ds, dg):
        flag = None
        if ds:
            flag = sfc < n_sfc - 1 if ds > 0 else sfc > 0
        if dg:
            extra = grp < n_grp - 1 if dg > 0 else grp > 0
            flag = extra if flag is None else jnp.logical_and(flag, extra)
        return flag

    gossip = n_sfc <= 9 and n_grp <= 4
    barrier = pltpu.get_barrier_semaphore()

    def place(i):
        peer = lax.rem(me + i, everyone)
        return peer, {"sfc": peer // n_grp, "grp": lax.rem(peer, n_grp)}

    def greet(i, carry):
        pl.semaphore_signal(barrier, inc=1, device_id=place(i)[1], device_id_type=MESH)
        return carry

    count_copy = pltpu.make_async_copy(count_hbm, counts, local_sem.at[0])
    source_copy = pltpu.make_async_copy(source_hbm, source_ref, local_sem.at[1])
    count_copy.start()
    source_copy.start()
    if gossip:
        for ds, dg in WAYS:
            @pl.when(there(ds, dg))
            def _(ds=ds, dg=dg):
                pl.semaphore_signal(
                    barrier, inc=1, device_id={"sfc": sfc + ds, "grp": grp + dg},
                    device_id_type=MESH,
                )
    else:
        lax.fori_loop(1, everyone, greet, 0)

    def one(flag):
        return jnp.where(flag, 1, 0)

    def greet_far(rnd, far):
        if gossip and far < n_sfc:
            for ds in (far, -far):
                @pl.when(sfc + ds < n_sfc if ds > 0 else sfc + ds >= 0)
                def _(ds=ds):
                    pl.semaphore_signal(
                        hello.at[rnd], inc=1, device_id={"sfc": sfc + ds}, device_id_type=MESH
                    )

    def hear_far(rnd, far):
        if gossip and far < n_sfc:
            pl.semaphore_wait(hello.at[rnd], one(sfc + far < n_sfc) + one(sfc >= far))

    lane = lax.broadcasted_iota(jnp.int32, (1, SUBS, LANES), 2)
    sub = lax.broadcasted_iota(jnp.int32, (1, SUBS, LANES), 1)
    z = lane % edge

    def has(flag_int):
        return flag_int > 0

    has_below = one(sfc > 0)
    has_above = one(sfc < n_sfc - 1)
    has_left = one(grp > 0)
    has_right = one(grp < n_grp - 1)
    owned = jnp.logical_and(sub >= middle, sub < middle + tiles)
    lefts = jnp.logical_and(sub >= middle - tiles, sub < middle)
    rights = jnp.logical_and(sub >= middle + tiles, sub < middle + 2 * tiles)
    rows_ok = (
        jnp.where(owned, 1, 0) + jnp.where(lefts, 1, 0) * has_left
        + jnp.where(rights, 1, 0) * has_right
    )
    def zero_rhs(i, carry):
        rhs[pl.ds(i * SUBS, SUBS), :] = jnp.zeros((SUBS, LANES), jnp.float32)
        return carry

    lax.fori_loop(0, planes + 2 * edge + 2, zero_rhs, 0)

    count_copy.wait()
    count = counts[0]
    for s in range(slots + 2):
        if s == 0:
            ok = has_below
        else:
            ok = one(count >= s) + one(count == s - 1) * has_above
        mask[pl.ds(SUBS * s, SUBS), :] = (rows_ok * ok).astype(jnp.float32)[0]

    for s in range(slots):
        mine = jnp.where(owned, 1, 0) * one(count > s)
        own[pl.ds(SUBS * s, SUBS), :] = mine.astype(jnp.float32)[0]

    def copies(e, i, ds, dg, src):
        gpos = 1 - dg
        if ds == 0:
            source, target = src, side.at[e, gpos // 2]
        else:
            tile, amount = ((0, 2), (1, 3), (3, 2))[dg + 1]
            source = packed.at[e, int(ds > 0), pl.ds(tile, amount)]
            target = (below if ds > 0 else above).at[e, gpos, pl.ds(0, amount)]
        return pltpu.make_async_remote_copy(
            src_ref=source, dst_ref=target, send_sem=send_sem.at[e, i],
            recv_sem=recv_sem.at[e, i], device_id={"sfc": sfc + ds, "grp": grp + dg},
            device_id_type=MESH,
        )

    def start(e, src):
        for i, (ds, dg) in enumerate(WAYS):
            @pl.when(there(ds, dg))
            def _(i=i, ds=ds, dg=dg):
                copies(e, i, ds, dg, src).start()

    def receive(e, src):
        for i, (ds, dg) in enumerate(WAYS):
            @pl.when(there(-ds, -dg))
            def _(i=i, ds=ds, dg=dg):
                copies(e, i, ds, dg, src).wait_recv()

    def sent(e, src):
        for i, (ds, dg) in enumerate(WAYS):
            @pl.when(there(ds, dg))
            def _(i=i, ds=ds, dg=dg):
                copies(e, i, ds, dg, src).wait_send()

    def pack(e, src):
        cut = SUBS // 2
        for up in (0, 1):
            rows = pl.ds(0, edge)
            value = [src[rows, pl.ds(t * LANES, LANES)] for t in range(tiles)]
            if up:
                for s in range(1, slots):
                    rows = pl.ds(s * edge, edge)
                    value = [
                        jnp.where(count > s, src[rows, pl.ds(t * LANES, LANES)], value[t])
                        for t in range(tiles)
                    ]
            if up:
                near = [v[edge - SUBS :] for v in value]
                far = [v[edge - SUBS - cut : edge - SUBS] for v in value]
                edges = [v[edge - cut :] for v in value]
            else:
                near = [v[:SUBS] for v in value]
                far = [v[SUBS : SUBS + cut] for v in value]
                edges = [v[:cut] for v in value]
            packed[e, up, 0] = jnp.concatenate([far[0], edges[1]], axis=0)
            packed[e, up, 1] = near[0]
            packed[e, up, 2] = jnp.concatenate([far[0], far[1]], axis=0)
            packed[e, up, 3] = near[1]
            packed[e, up, 4] = jnp.concatenate([far[1], edges[0]], axis=0)

    def ghost(ref, e, up, g, h, t):
        cut = SUBS // 2
        near_h = 1 if up else 0
        if g == 1:
            if h == near_h:
                return ref[e, g, 0 if t == 0 else 2]
            mix, low = ref[e, g, 1], t == 0
        else:
            full = 1 if g == 0 else 0
            if h == near_h and t == full:
                return ref[e, g, 0 if g == 0 else 1]
            mix = ref[e, g, 1 if g == 0 else 0]
            if h == near_h:
                low = False
            elif t == full:
                low = True
            else:
                return jnp.zeros((SUBS, LANES), jnp.float32)
        half = mix[:cut] if low else mix[cut:]
        none = jnp.zeros((cut, LANES), jnp.float32)
        return jnp.concatenate([none, half] if up else [half, none], axis=0)

    def unpack(e, src):
        sides = ((0, has_left), (1, 1), (2, has_right))
        for g, present in sides:
            for s in range(slots + 2):
                for h in range(edge // SUBS):
                    for t in range(tiles):
                        cols = pl.ds(t * LANES, LANES)
                        rows = pl.ds(h * SUBS, SUBS)

                        def centre(slot):
                            at = pl.ds(slot * edge + h * SUBS, SUBS)
                            return src[at, cols] if g == 1 else side[e, g // 2, at, cols]

                        if s == 0:
                            value = jnp.where(has(has_below * present), ghost(below, e, 1, g, h, t), 0.0)
                        else:
                            up = one(count == s - 1) * has_above * present
                            value = jnp.zeros((SUBS, LANES), jnp.float32)
                            if s >= 2:
                                value = jnp.where(has(up), ghost(above, e, 0, g, h, t), value)
                            if s <= slots:
                                value = jnp.where(has(one(count >= s) * present), centre(s - 1), value)
                        plane = 1 + s * edge + h * SUBS
                        at_sub = middle + (g - 1) * tiles + t
                        rhs[pl.ds(plane * SUBS + at_sub, SUBS, stride=SUBS), :] = value

    def roll(v, amount, axis):
        return pltpu.roll(v, amount % v.shape[axis], axis)

    def inplane(v, dz, dy):
        up_z = jnp.where(z < edge - dz, roll(v, -dz, 2), 0.0)
        down_z = jnp.where(z >= dz, roll(v, dz, 2), 0.0)
        ru = roll(v, -dy, 2)
        up_y = jnp.where(lane < LANES - dy, ru, roll(ru, -1, 1))
        rd = roll(v, dy, 2)
        down_y = jnp.where(lane >= dy, rd, roll(rd, 1, 1))
        return (up_z + down_z) + (up_y + down_y)

    def load(ref, p, n):
        return ref[pl.ds((p + 1) * SUBS, n * SUBS), :].reshape(n, SUBS, LANES)

    def store(ref, p, value):
        n = value.shape[0]
        ref[pl.ds((p + 1) * SUBS, n * SUBS), :] = value.reshape(n * SUBS, LANES)

    def lap(ref, p, n, dz=1, dy=edge):
        wide = load(ref, p - 1, n + 2)
        v = wide[1:-1]
        return v, 6.0 * v - (wide[:-2] + wide[2:]) - inplane(v, dz, dy)

    def slot_mask(s):
        return mask[pl.ds(SUBS * s, SUBS), :][None]

    chunk = SUBS
    per_slot = edge // chunk
    chunks = (slots + 2) * per_slot

    def vcycle(on_sum=None):
        acc = jnp.zeros((SUBS, LANES), jnp.float32)
        for c in range(chunks):
            r, applied = lap(rhs, c * chunk, chunk)
            store(smooth, c * chunk, slot_mask(c // per_slot) * (2.0 * step * r - step * step * applied))
        for c in range(chunks):
            v, applied = lap(smooth, c * chunk, chunk)
            r = load(rhs, c * chunk, chunk)
            q = r - applied
            s = c // per_slot - 1
            if on_sum is not None and 0 <= s < slots:
                acc = acc + own[pl.ds(SUBS * s, SUBS), :] * jnp.sum((r + q) * v, axis=0)
            q = q.reshape(chunk // 2, 2, SUBS, LANES)
            q = q[:, 0] + q[:, 1]
            q = q + jnp.where(lane % 2 == 0, roll(q, -1, 2), roll(q, 1, 2))
            q = q + jnp.where(lane // edge % 2 == 0, roll(q, -edge, 2), roll(q, edge, 2))
            store(coarse, c * chunk // 2, slot_mask(c // per_slot) * (0.125 * q))
        half = edge // 2
        for s in range(slots + 2):
            v, applied = lap(coarse, s * half, half, 2, 2 * edge)
            store(ea, s * half, slot_mask(s) * (2.0 * cstep * v - 0.25 * cstep * cstep * applied))
        now, then = ea, eb
        for sweep in range(COARSE_SWEEPS - 2):
            for s in range(slots + 2):
                v, applied = lap(now, s * half, half, 2, 2 * edge)
                c = load(coarse, s * half, half)
                value = slot_mask(s) * (v + cstep * (c - 0.25 * applied))
                store(then, s * half, value)
            now, then = then, now
        if on_sum is not None:
            for s in range(slots):
                ce = load(coarse, (s + 1) * half, half) * load(now, (s + 1) * half, half)
                acc = acc + own[pl.ds(SUBS * s, SUBS), :] * (2.0 * jnp.sum(ce, axis=0))
            on_sum(acc)
        for c in range(1, chunks - 1):
            e = load(now, c * chunk // 2, chunk // 2)[:, None]
            e = jnp.broadcast_to(e, (chunk // 2, 2, SUBS, LANES)).reshape(chunk, SUBS, LANES)
            store(smooth, c * chunk, load(smooth, c * chunk, chunk) + e)
        now, then = smooth, other
        for sweep in range(POST_SWEEPS):
            for c in range(1, chunks - 1):
                v, applied = lap(now, c * chunk, chunk)
                r = load(rhs, c * chunk, chunk)
                store(then, c * chunk, slot_mask(c // per_slot) * (v + step * (r - applied)))
            now, then = then, now
        return now

    def natural(ref, s, h, t):
        plane = 1 + (s + 1) * edge + h * SUBS
        return ref[pl.ds(plane * SUBS + middle + t, SUBS, stride=SUBS), :]

    def owned_tiles():
        for s in range(slots):
            for h in range(edge // SUBS):
                for t in range(tiles):
                    yield s, h, t, pl.ds(s * edge + h * SUBS, SUBS), pl.ds(t * LANES, LANES)

    source_copy.wait()
    pack(0, source_ref)
    if gossip:
        near = (1 + one(sfc > 0) + one(sfc < n_sfc - 1)) * (1 + one(grp > 0) + one(grp < n_grp - 1))
        pl.semaphore_wait(barrier, near - 1)
    else:
        pl.semaphore_wait(barrier, everyone - 1)
    start(0, source_ref)
    receive(0, source_ref)
    greet_far(0, 2)
    unpack(0, source_ref)
    z0 = vcycle()
    for c in range(per_slot, chunks - per_slot):
        _, applied = lap(z0, c * chunk, chunk)
        store(other, c * chunk, applied)
    acc_rz = jnp.zeros((SUBS, LANES), jnp.float32)
    acc_curv = jnp.zeros((SUBS, LANES), jnp.float32)
    for s, h, t, rows, cols in owned_tiles():
        value = natural(z0, s, h, t)
        image = natural(other, s, h, t)
        source = source_ref[rows, cols]
        if s:
            value = jnp.where(count > s, value, 0.0)
            image = jnp.where(count > s, image, 0.0)
            source = jnp.where(count > s, source, 0.0)
        first_ref[rows, cols] = value
        image_ref[rows, cols] = image
        image_buf[rows, cols] = image
        source_out[rows, cols] = source
        acc_rz = acc_rz + source * value
        acc_curv = acc_curv + value * image
    pack(1, image_buf)
    hear_far(0, 2)
    start(1, image_buf)
    row = lax.broadcasted_iota(jnp.int32, (1, LANES), 1)

    def whole(acc):
        return jnp.sum(jnp.sum(acc, axis=0, keepdims=True), axis=1, keepdims=True)

    rz, curv = whole(acc_rz), whole(acc_curv)
    known = jnp.where(row == 0, rz, jnp.where(row == 1, curv, 0.0))
    receive(1, image_buf)
    greet_far(1, 4)
    unpack(1, image_buf)

    def send(slot, peer, device):
        return pltpu.make_async_remote_copy(
            src_ref=part, dst_ref=red.at[slot], send_sem=red_send.at[peer],
            recv_sem=red_recv.at[slot], device_id=device, device_id_type=MESH,
        )

    def spread(acc):
        value = jnp.where(row == 2, whole(acc), known)
        part[...] = value
        red[me] = value
        hear_far(1, 4)

        def go(i, carry):
            peer, device = place(i)
            send(me, peer, device).start()
            return carry

        lax.fori_loop(1, everyone, go, 0)

    w = vcycle(spread)
    for s, h, t, rows, cols in owned_tiles():
        value = natural(w, s, h, t)
        if s:
            value = jnp.where(count > s, value, 0.0)
        w_ref[rows, cols] = value
    sent(0, source_ref)
    sent(1, image_buf)

    def got(i, carry):
        peer, device = place(i)
        send(peer, peer, device).wait_recv()
        return carry

    lax.fori_loop(1, everyone, got, 0)
    sums = jnp.sum(red[...], axis=0)

    def pick(i):
        return jnp.sum(jnp.where(row == i, sums, 0.0), axis=1, keepdims=True)

    alpha = pick(0) / pick(1)
    ratio = pick(2) / pick(1)
    scale_ref[...] = jnp.concatenate(
        [jnp.broadcast_to(alpha, (1, LANES)), jnp.broadcast_to(ratio, (1, LANES))], axis=0
    )

    def out(i, carry):
        peer, device = place(i)
        send(me, peer, device).wait_send()
        return carry

    lax.fori_loop(1, everyone, out, 0)


def combine(first, image, w, source, scale, solution_ref, residual_ref, direction_ref):
    alpha = scale[0:1, 0:1]
    ratio = scale[1:2, 0:1]
    solution_ref[...] = alpha * first[...]
    residual_ref[...] = source[...] - alpha * image[...]
    direction_ref[...] = alpha * (ratio * first[...] - w[...])


def shards(n_sfc, n_grp, source, layer_counts):
    slots, edge, width = source.shape
    planes, tiles = slots * edge, width // LANES
    padded = (planes + 2 * edge + 2) * SUBS
    half_padded = ((slots + 2) * edge // 2 + 2) * SUBS
    f32 = jnp.float32
    vmem = pltpu.VMEM
    dma = pltpu.SemaphoreType.DMA
    n = n_sfc * n_grp
    out = jax.ShapeDtypeStruct((planes, width), f32)
    parts = pl.pallas_call(
        functools.partial(kernel, (slots, edge, tiles, n_sfc, n_grp)),
        out_shape=(out, out, out, out, jax.ShapeDtypeStruct((2, LANES), f32)),
        in_specs=[pl.BlockSpec(memory_space=pl.ANY)] * 2,
        out_specs=[pl.BlockSpec(memory_space=pltpu.VMEM)] * 5,
        scratch_shapes=[
            vmem((planes, width), f32),
            vmem((planes, width), f32),
            pltpu.SMEM((1,), jnp.int32),
            vmem((padded, LANES), f32),
            vmem((padded, LANES), f32),
            vmem((padded, LANES), f32),
            vmem((half_padded, LANES), f32),
            vmem((half_padded, LANES), f32),
            vmem((half_padded, LANES), f32),
            vmem(((slots + 2) * SUBS, LANES), f32),
            vmem((slots * SUBS, LANES), f32),
            vmem((2, 2, 5, SUBS, LANES), f32),
            vmem((2, 2, planes, width), f32),
            vmem((2, 3, 3, SUBS, LANES), f32),
            vmem((2, 3, 3, SUBS, LANES), f32),
            vmem((1, LANES), f32),
            vmem((n, 1, LANES), f32),
            dma((2,)),
            dma((2, len(WAYS))),
            dma((2, len(WAYS))),
            dma((n,)),
            dma((n,)),
            pltpu.SemaphoreType.REGULAR((2,)),
        ],
        compiler_params=pltpu.CompilerParams(
            collective_id=0, has_side_effects=True, vmem_limit_bytes=16 * 1024 * 1024
        ),
        name="pcg",
    )(layer_counts, source.reshape(planes, width))
    outs = pl.pallas_call(
        combine,
        out_shape=(out, out, out),
        in_specs=[pl.BlockSpec(memory_space=pltpu.VMEM)] * 5,
        out_specs=[pl.BlockSpec(memory_space=pltpu.VMEM)] * 3,
        compiler_params=pltpu.CompilerParams(vmem_limit_bytes=16 * 1024 * 1024),
        name="combine",
    )(*parts)
    return tuple(o.reshape(source.shape) for o in outs)


def solution(mesh):
    n_sfc, n_grp = mesh.shape["sfc"], mesh.shape["grp"]
    return jax.shard_map(
        functools.partial(shards, n_sfc, n_grp),
        mesh=mesh,
        in_specs=(P("sfc", None, "grp"), P("sfc")),
        out_specs=(P("sfc", None, "grp"), P("sfc", None, "grp"), P("sfc", None, "grp")),
        check_vma=False,
    )
```
